512 devices in a mesh: grp: 2 (over y), seq: 128 (over x, z), bat: 2 (over core).
Axes of the slice: x: 8, y: 2, z: 16, core: 2. Of those that a mesh axis runs over, the one named last changes fastest.
The devices are a block of a 8x8x16 slice.
Arguments:
- queries: bfloat16 [16, 16, 192], P(('grp', 'bat')), parts along dimension 0, may hold values from -8 to 8
- latent_cache: bfloat16 [16, 65536, 576], P('grp', 'seq'), parts along dimension 0, may hold values from -128 to 128
- cache_lengths: int32 [16], P('grp'), parts along dimension 0, may hold values from 128 to 65536, as said below
- key_weight: bfloat16 [16, 128, 512], P('bat'), may hold values from -0.5 to 0.5
- value_weight: bfloat16 [16, 512, 128], P('bat'), may hold values from -0.25 to 0.25
Outputs:
- attended: bfloat16 [16, 16, 128], P(('grp', 'bat')), parts along dimension 0
The draws below stay inside these ranges and needn't reach their ends.
There are 2 independent parts, one for each index of `grp`. The reference program is written for one: setup_inputs(seed, part) draws one part's arguments, and reference() takes and returns one part's arrays. A program takes and returns all parts, laid end to end along the dimension named above; an argument that names none is the same for every part. Nothing has to cross between parts.
Inputs may be any that keep to these rules, and one draw needn't show every extreme that they name: `cache_lengths`: each entry is a multiple of 128; at least one request has all 65536 positions valid and at least one has fewer.
All inputs are finite; a program needn't handle non-finite values.
Results may differ from the reference program's by a relative error of at most 0.0085.
Values may be sent and summed in bfloat16 or wider, within the bound.
No kernel may reach another device: no remote copies, remote signals or barrier semaphores. Data moves between devices by JAX's collectives and lax.ppermute only.
A program may use at most 64 MiB of HBM per device.

```python
import jax
import jax.numpy as jnp
from jax import lax

H = 16
DC = 512
DR = 64
DN = 128
DV = 128
REQ = 8
SEQ = 65536


def query_table(key):
    base_key = jax.random.fold_in(key, 101)
    values_all = 1.8 * jax.random.normal(base_key, (REQ, H, DN + DR), jnp.float32)
    return jnp.clip(values_all, -8.0, 8.0)


def draw_queries(key, part):
    return query_table(key).astype(jnp.bfloat16)


def draw_latent_cache(key, part):
    base_key = jax.random.fold_in(key, 202)
    values_all = jax.random.normal(base_key, (REQ, SEQ, DC + DR), jnp.float32)
    values_all = jnp.clip(values_all, -6.0, 6.0)
    return values_all.astype(jnp.bfloat16)


def draw_cache_lengths(key, part):
    blocks = SEQ // 128
    request_ids = jnp.arange(REQ, dtype=jnp.int32)
    blocks_used = jax.random.randint(jax.random.fold_in(key, 303), (REQ,), 1, blocks + 1)
    longest = jax.random.randint(jax.random.fold_in(key, 304), (), 0, REQ)
    offset = jax.random.randint(jax.random.fold_in(key, 305), (), 1, REQ)
    shortest = (longest + offset) % REQ
    short_blocks = jax.random.randint(jax.random.fold_in(key, 306), (), 1, blocks)
    blocks_used = jnp.where(request_ids == shortest, short_blocks, blocks_used)
    blocks_used = jnp.where(request_ids == longest, blocks, blocks_used)
    return (blocks_used * 128).astype(jnp.int32)


def block_levels(stream_key, shape, pieces, smallest, high):
    loudness, own = 1.0, jax.random.fold_in(stream_key, 6)
    for dim, shards_of in pieces:
        draws = jnp.exp(jax.random.uniform(jax.random.fold_in(own, dim), (shards_of,), jnp.float32, smallest / len(pieces), high / len(pieces)))
        loudness = loudness * jnp.repeat(draws, shape[dim] // shards_of).reshape([-1 if axis == dim else 1 for axis in range(len(shape))])
    return loudness


def gaussian(rng, dims, width, limit, pieces=(), kind=jnp.bfloat16):
    result = width * jax.random.normal(rng, dims, jnp.float32)
    if pieces:
        result = result * block_levels(rng, dims, pieces, -0.22, 0.18)
    return jnp.clip(result, -limit, limit).astype(kind)


def setup_inputs(seed: int = 0, part: int = 0) -> dict:
    seeds = jax.random.split(jax.random.key(seed), 6)
    part_splits = jax.random.split(jax.random.fold_in(seeds[5], part), 6)
    return {
        "queries": draw_queries(jax.random.fold_in(jax.random.fold_in(seeds[5], part), 71), part),
        "latent_cache": draw_latent_cache(jax.random.fold_in(jax.random.fold_in(seeds[5], part), 71), part),
        "cache_lengths": draw_cache_lengths(jax.random.fold_in(jax.random.fold_in(seeds[5], part), 71), part),
        "key_weight": gaussian(seeds[3], (H, DN, DC), DN ** -0.5, 0.5, ((0, 2),)),
        "value_weight": gaussian(seeds[4], (H, DC, DV), DC ** -0.5, 0.25, ((0, 2),)),
    }


def reference(queries, latent_cache, cache_lengths, key_weight, value_weight):
    scaling = (DN + DR) ** -0.5
    positions = jnp.arange(SEQ, dtype=jnp.int32)
    key_full = key_weight.astype(jnp.float32)
    value_full = value_weight.astype(jnp.float32)

    def single(inputs):
        query_row, cache_rows, length = inputs
        absorbed = jnp.einsum("hd,hdc->hc", query_row[:, :DN].astype(jnp.float32), key_full).astype(jnp.bfloat16)
        joined = jnp.concatenate([absorbed, query_row[:, DN:]], axis=1)
        scores = lax.dot_general(joined, cache_rows, (((1,), (1,)), ((), ())), preferred_element_type=jnp.float32) * scaling
        scores = jnp.where((positions < length)[None, :], scores, -jnp.inf)
        maxima = jnp.max(scores, axis=1, keepdims=True)
        weights = jnp.exp(scores - maxima)
        totals = jnp.sum(weights, axis=1, keepdims=True)
        latent_out = jnp.dot(weights.astype(jnp.bfloat16), cache_rows[:, :DC], preferred_element_type=jnp.float32) / totals
        projected = jnp.einsum("hc,hcd->hd", latent_out, value_full, precision=lax.Precision.HIGHEST)
        return projected.astype(jnp.bfloat16)

    return lax.map(single, (queries, latent_cache, cache_lengths))
```

```python
import functools

import jax
import jax.numpy as jnp
from jax import lax
from jax.experimental import pallas as pl
from jax.experimental.pallas import tpu as pltpu
from jax.sharding import Mesh
from jax.sharding import PartitionSpec as P

SEQ = ("seq_0", "seq_1")
SEQ_0 = 8
BAT = 2

masked_score = -1e30
lanes = 128
terms = 3
small_grant = 8 * 2**20
large_grant = 51 * 2**20


def split_terms(value):
    parts = []
    for _ in range(terms):
        part = value.astype(jnp.bfloat16).astype(jnp.float32)
        parts.append(part)
        value = value - part
    return parts


def put_stats(stats, k, width, maxima, totals):
    lane = lax.broadcasted_iota(jnp.int32, stats.shape, 1)
    for i, part in enumerate(split_terms(maxima) + split_terms(totals)):
        stats = jnp.where(lane == i * width + k, part, stats)
    return stats


def take_stats(stats, width):
    parts = [stats[..., i * width : (i + 1) * width] for i in range(2 * terms)]
    return (parts[0] + parts[1] + parts[2], parts[3] + parts[4] + parts[5])


def attend_kernel(scaling, lengths, start, query, cache, value, out, latent, keys, arrived):
    requests, heads = query.shape[:2]
    latent_width, shard_len = value.shape[1], cache.shape[2]
    own = requests // BAT
    copies = [
        pltpu.make_async_copy(cache.at[r], keys.at[r], arrived.at[r]) for r in range(requests)
    ]
    for copy in copies:
        copy.start()
    positions = start[0] + lax.broadcasted_iota(jnp.int32, (heads, shard_len), 1)
    stats = [jnp.zeros((heads, lanes), jnp.float32) for _ in range(BAT)]
    for r in range(requests):
        copies[r].wait()
        scores = jnp.dot(query[r], keys[r], preferred_element_type=jnp.float32) * scaling
        scores = jnp.where(positions < lengths[r], scores, masked_score)
        maxima = jnp.max(scores, axis=1, keepdims=True)
        weights = jnp.exp(scores - maxima)
        totals = jnp.sum(weights, axis=1, keepdims=True)
        latent[:, r, :] = lax.dot_general(
            weights.astype(jnp.bfloat16),
            keys[r, :latent_width],
            (((1,), (1,)), ((), ())),
            preferred_element_type=jnp.float32,
        )
        stats[r // own] = put_stats(stats[r // own], r % own, own, maxima, totals)
    projected = [
        jnp.dot(latent[h].astype(jnp.bfloat16), value[h], preferred_element_type=jnp.float32)
        for h in range(heads)
    ]
    projected = jnp.stack(projected, axis=1)
    for b in range(BAT):
        block = projected[b * own : (b + 1) * own].reshape(own * heads, lanes)
        block = jnp.concatenate([block, stats[b]], axis=0).astype(jnp.bfloat16)
        for x in range(out.shape[0]):
            out[x, b] = block


def attend(joined, cache, lengths, start, value, scaling, copies):
    requests, heads, _ = joined.shape
    turned = jnp.swapaxes(cache, 1, 2)
    vmem, smem = pl.BlockSpec(memory_space=pltpu.VMEM), pl.BlockSpec(memory_space=pltpu.SMEM)
    return pl.pallas_call(
        functools.partial(attend_kernel, scaling),
        out_shape=jax.ShapeDtypeStruct(
            (copies, BAT, (requests // BAT + 1) * heads, lanes), jnp.bfloat16
        ),
        in_specs=[smem, smem, vmem, pl.BlockSpec(memory_space=pltpu.HBM), vmem],
        out_specs=vmem,
        scratch_shapes=[
            pltpu.VMEM((heads, requests, value.shape[1]), jnp.float32),
            pltpu.VMEM(turned.shape, turned.dtype),
            pltpu.SemaphoreType.DMA((requests,)),
        ],
        compiler_params=pltpu.CompilerParams(vmem_limit_bytes=large_grant),
        name="attend",
    )(lengths, start, joined, turned, value)


def merged(tiles, stats, width):
    heads = stats.shape[1]
    maxima, totals = take_stats(stats, width)
    highest = jnp.max(maxima, axis=0, keepdims=True)
    factors = jnp.exp(maxima - highest)
    total = jnp.sum(totals * factors, axis=0)
    sums = []
    for k in range(width):
        part = tiles[:, k * heads : (k + 1) * heads] * factors[:, :, k : k + 1]
        sums.append(jnp.sum(part, axis=0))
    return sums, highest[0], total


def merge_kernel(heads, pieces, out):
    copies = out.shape[0]
    rows = pieces.shape[2]
    width = rows // heads - 1
    for b in range(BAT):
        block = pieces[:, b].astype(jnp.float32)
        sums, highest, total = merged(block[:, : width * heads], block[:, width * heads :], width)
        stats = jnp.zeros((heads, lanes), jnp.float32)
        for k in range(width):
            stats = put_stats(stats, k, width, highest[:, k : k + 1], total[:, k : k + 1])
        result = jnp.concatenate([*sums, stats], axis=0).astype(jnp.bfloat16)
        for c in range(copies):
            out[c, b] = result


def finish_kernel(heads, pieces, out):
    rows = pieces.shape[2]
    width = rows // heads - 1
    for b in range(BAT):
        block = pieces[:, b].astype(jnp.float32)
        sums, _, total = merged(block[:, : width * heads], block[:, width * heads :], width)
        for k in range(width):
            out[k, b] = (sums[k] / total[:, k : k + 1]).astype(jnp.bfloat16)


def whole(kernel, shape, name, operand):
    return pl.pallas_call(
        kernel,
        out_shape=jax.ShapeDtypeStruct(shape, jnp.bfloat16),
        in_specs=[pl.BlockSpec(memory_space=pltpu.VMEM)],
        out_specs=pl.BlockSpec(memory_space=pltpu.VMEM),
        compiler_params=pltpu.CompilerParams(vmem_limit_bytes=small_grant),
        name=name,
    )(operand)


def per_device(queries, latent_cache, cache_lengths, key_weight, value_weight):
    nope_width = key_weight.shape[1]
    heads = key_weight.shape[0]
    grouped = lax.all_to_all(queries, "bat", split_axis=1, concat_axis=0, tiled=True)
    absorbed = jnp.einsum(
        "bhd,hdc->bhc", grouped[:, :, :nope_width], key_weight, preferred_element_type=jnp.float32
    ).astype(jnp.bfloat16)
    joined = jnp.concatenate([absorbed, grouped[:, :, nope_width:]], axis=2)
    scaling = queries.shape[2] ** (-0.5)
    shard_len = latent_cache.shape[1]
    start = (lax.axis_index(SEQ) * shard_len).astype(jnp.int32).reshape(1)
    across, along = lax.axis_size("seq_0"), lax.axis_size("seq_1")
    partial = attend(joined, latent_cache, cache_lengths, start, value_weight, scaling, across)
    shape = partial.shape
    pieces = lax.all_to_all(
        partial.reshape(across * BAT, *shape[2:]), ("seq_0", "bat"), 0, 0, tiled=True
    ).reshape(shape)
    partial = whole(
        functools.partial(merge_kernel, heads), (along, *shape[1:]), "merge_across", pieces
    )
    pieces = lax.all_to_all(partial, "seq_1", 0, 0, tiled=True)
    own = queries.shape[0]
    result = whole(
        functools.partial(finish_kernel, heads),
        (own, BAT, heads, value_weight.shape[2]),
        "finish",
        pieces,
    )
    return result.reshape(own, BAT * heads, value_weight.shape[2])


def solution(mesh):
    torus = Mesh(
        mesh.devices.reshape(mesh.shape["grp"], SEQ_0, mesh.shape["seq"] // SEQ_0, mesh.shape["bat"]),
        ("grp", "seq_0", "seq_1", "bat"),
    )
    placed = (
        P(("grp", "bat"), None, None),
        P("grp", SEQ, None),
        P("grp"),
        P("bat", None, None),
        P("bat", None, None),
    )
    return jax.shard_map(
        per_device,
        mesh=torus,
        in_specs=placed,
        out_specs=P(("grp", "bat"), None, None),
        check_vma=False,
    )
```

```python
import functools

import jax
import jax.numpy as jnp
from jax import lax
from jax.experimental import pallas as pl
from jax.experimental.pallas import tpu as pltpu
from jax.sharding import Mesh
from jax.sharding import PartitionSpec as P


SEQ = ("seq_0", "seq_1")
SEQ_0 = 8
BAT = 2

masked_score = -1e30
empty_score = -3e38
lanes = 128
terms = 3
small_grant = 8 * 2**20
large_grant = 51 * 2**20


def split_terms(value):
    parts = []
    for _ in range(terms):
        part = value.astype(jnp.bfloat16).astype(jnp.float32)
        parts.append(part)
        value = value - part
    return parts


def put_stats(stats, k, width, maxima, totals):
    lane = lax.broadcasted_iota(jnp.int32, stats.shape, 1)
    for i, part in enumerate(split_terms(maxima) + split_terms(totals)):
        stats = jnp.where(lane == i * width + k, part, stats)
    return stats


def take_stats(stats, width):
    parts = [stats[..., i * width : (i + 1) * width] for i in range(2 * terms)]
    return (parts[0] + parts[1] + parts[2], parts[3] + parts[4] + parts[5])


def attend_kernel(scaling, lengths, start, query, cache, value, out, latent, keys, arrived):
    requests, heads = query.shape[:2]
    latent_width, shard_len = value.shape[1], cache.shape[2]
    own = requests // BAT
    copies = [
        pltpu.make_async_copy(cache.at[r], keys.at[r], arrived.at[r]) for r in range(requests)
    ]
    for copy in copies:
        copy.start()
    positions = start[0] + lax.broadcasted_iota(jnp.int32, (heads, shard_len), 1)
    stats = [jnp.zeros((heads, lanes), jnp.float32) for _ in range(BAT)]
    for r in range(requests):
        copies[r].wait()
        scores = jnp.dot(query[r], keys[r], preferred_element_type=jnp.float32) * scaling
        scores = jnp.where(positions < lengths[r], scores, masked_score)
        maxima = jnp.max(scores, axis=1, keepdims=True)
        weights = jnp.exp(scores - maxima)
        totals = jnp.sum(weights, axis=1, keepdims=True)
        latent[:, r, :] = lax.dot_general(
            weights.astype(jnp.bfloat16),
            keys[r, :latent_width],
            (((1,), (1,)), ((), ())),
            preferred_element_type=jnp.float32,
        )
        stats[r // own] = put_stats(stats[r // own], r % own, own, maxima, totals)
    projected = [
        jnp.dot(latent[h].astype(jnp.bfloat16), value[h], preferred_element_type=jnp.float32)
        for h in range(heads)
    ]
    projected = jnp.stack(projected, axis=1)
    for b in range(BAT):
        block = projected[b * own : (b + 1) * own].reshape(own * heads, lanes)
        block = jnp.concatenate([block, stats[b]], axis=0).astype(jnp.bfloat16)
        for x in range(out.shape[0]):
            out[x, b] = block


def attend(joined, cache, lengths, start, value, scaling, copies):
    requests, heads, _ = joined.shape
    turned = jnp.swapaxes(cache, 1, 2)
    vmem, smem = pl.BlockSpec(memory_space=pltpu.VMEM), pl.BlockSpec(memory_space=pltpu.SMEM)
    return pl.pallas_call(
        functools.partial(attend_kernel, scaling),
        out_shape=jax.ShapeDtypeStruct(
            (copies, BAT, (requests // BAT + 1) * heads, lanes), jnp.bfloat16
        ),
        in_specs=[smem, smem, vmem, pl.BlockSpec(memory_space=pltpu.HBM), vmem],
        out_specs=vmem,
        scratch_shapes=[
            pltpu.VMEM((heads, requests, value.shape[1]), jnp.float32),
            pltpu.VMEM(turned.shape, turned.dtype),
            pltpu.SemaphoreType.DMA((requests,)),
        ],
        compiler_params=pltpu.CompilerParams(vmem_limit_bytes=large_grant),
        name="attend",
    )(lengths, start, joined, turned, value)


def merged(tiles, stats, width):
    heads = stats.shape[1]
    maxima, totals = take_stats(stats, width)
    maxima = jnp.where(totals > 0, maxima, empty_score)
    highest = jnp.max(maxima, axis=0, keepdims=True)
    factors = jnp.exp(maxima - highest)
    total = jnp.sum(totals * factors, axis=0)
    sums = []
    for k in range(width):
        part = tiles[:, k * heads : (k + 1) * heads] * factors[:, :, k : k + 1]
        sums.append(jnp.sum(part, axis=0))
    return sums, highest[0], total


def summed(heads, pieces):
    width = pieces.shape[1] // heads - 1
    block = pieces.astype(jnp.float32)
    return merged(block[:, : width * heads], block[:, width * heads :], width)


def packed(heads, sums, highest, total):
    stats = jnp.zeros((heads, lanes), jnp.float32)
    for k in range(len(sums)):
        stats = put_stats(stats, k, len(sums), highest[:, k : k + 1], total[:, k : k + 1])
    return jnp.concatenate([*sums, stats], axis=0).astype(jnp.bfloat16)


def merge_across_kernel(heads, pieces, out):
    for b in range(BAT):
        out[b] = packed(heads, *summed(heads, pieces[:, b]))


def merge_kernel(heads, *refs):
    *parts, out = refs
    for b in range(BAT):
        out[b] = packed(heads, *summed(heads, jnp.stack([part[b] for part in parts])))


def finish_kernel(heads, *refs):
    *parts, out = refs
    for b in range(BAT):
        sums, _, total = summed(heads, jnp.stack([part[b] for part in parts]))
        for k in range(len(sums)):
            out[k, b] = (sums[k] / total[:, k : k + 1]).astype(jnp.bfloat16)


def whole(kernel, heads, shape, name, *operands):
    vmem = pl.BlockSpec(memory_space=pltpu.VMEM)
    return pl.pallas_call(
        functools.partial(kernel, heads),
        out_shape=jax.ShapeDtypeStruct(shape, jnp.bfloat16),
        in_specs=[vmem] * len(operands),
        out_specs=vmem,
        compiler_params=pltpu.CompilerParams(vmem_limit_bytes=small_grant),
        name=name,
    )(*operands)


def moved(value, pairs):
    return lax.ppermute(value, "seq_1", pairs)


def one_of(plane, planes):
    return functools.reduce(jnp.logical_or, [plane == p for p in planes])


def within(plane, planes, step, value):
    return lax.cond(one_of(plane, planes), step, lambda kept: kept, value)


def gathered_at_first(plane, last, partial, heads, shape):
    merge = functools.partial(whole, merge_kernel, heads, partial.shape, "merge")

    def folded(pairs):
        return lambda kept: merge(kept, moved(kept, pairs))

    def tree(kept):
        kept = within(plane, range(2, 10), folded([(9, 8), (7, 6), (5, 4), (3, 2)]), kept)
        kept = within(plane, (4, 6), folded([(6, 4)]), kept)
        kept = within(plane, (2, 4), folded([(4, 2)]), kept)
        sources = [2, 8, *range(10, last - 1)]

        def collect(kept):
            return merge(kept, *[moved(kept, [(p, 1)]) for p in sources])

        return within(plane, (1, *sources), collect, kept)

    partial = within(plane, range(1, last - 1), tree, partial)

    def finish(kept):
        parts = [moved(kept, [(p, 0)]) for p in (last - 1, 1, last)]
        return whole(finish_kernel, heads, shape, "finish", kept, *parts)

    planes = (0, 1, last - 1, last)
    return lax.cond(
        one_of(plane, planes), finish, lambda _: jnp.zeros(shape, jnp.bfloat16), partial
    )


def handed_on(plane, result):
    rounds = (
        ([(0, 1)],),
        ([(1, 2)], [(1, 3)]),
        ([(2, 4)],),
        ([(3, 5), (4, 7)], [(3, 6), (4, 8)]),
        ([(5, 9), (6, 11), (7, 13), (8, 15)], [(5, 10), (6, 12), (7, 14)]),
    )
    for moves in rounds:

        def step(kept, moves=moves):
            arrived = [moved(kept, pairs) for pairs in moves]
            for value, pairs in zip(arrived, moves):
                kept = jnp.where(one_of(plane, [target for _, target in pairs]), value, kept)
            return kept

        planes = sorted({p for pairs in moves for pair in pairs for p in pair})
        result = within(plane, planes, step, result)
    return result


def per_device(queries, latent_cache, cache_lengths, key_weight, value_weight):
    nope_width = key_weight.shape[1]
    heads = key_weight.shape[0]
    grouped = lax.all_to_all(queries, "bat", split_axis=1, concat_axis=0, tiled=True)
    absorbed = jnp.einsum(
        "bhd,hdc->bhc", grouped[:, :, :nope_width], key_weight, preferred_element_type=jnp.float32
    ).astype(jnp.bfloat16)
    joined = jnp.concatenate([absorbed, grouped[:, :, nope_width:]], axis=2)
    scaling = queries.shape[2] ** (-0.5)
    shard_len = latent_cache.shape[1]
    start = (lax.axis_index(SEQ) * shard_len).astype(jnp.int32).reshape(1)
    across, along = lax.axis_size("seq_0"), lax.axis_size("seq_1")
    partial = attend(joined, latent_cache, cache_lengths, start, value_weight, scaling, across)
    shape = partial.shape
    pieces = lax.all_to_all(
        partial.reshape(across * BAT, *shape[2:]), ("seq_0", "bat"), 0, 0, tiled=True
    ).reshape(shape)
    partial = whole(merge_across_kernel, heads, shape[1:], "merge_across", pieces)
    plane = lax.axis_index("seq_1")
    own, value_width = queries.shape[0], value_weight.shape[2]
    result = gathered_at_first(plane, along - 1, partial, heads, (own, BAT, heads, value_width))
    result = handed_on(plane, result)
    return result.reshape(own, BAT * heads, value_width)


def solution(mesh):
    torus = Mesh(
        mesh.devices.reshape(mesh.shape["grp"], SEQ_0, mesh.shape["seq"] // SEQ_0, mesh.shape["bat"]),
        ("grp", "seq_0", "seq_1", "bat"),
    )
    placed = (
        P(("grp", "bat"), None, None),
        P("grp", SEQ, None),
        P("grp"),
        P("bat", None, None),
        P("bat", None, None),
    )
    return jax.shard_map(
        per_device,
        mesh=torus,
        in_specs=placed,
        out_specs=P(("grp", "bat"), None, None),
        check_vma=False,
    )
```

```python
import functools

import jax
import jax.numpy as jnp
from jax import lax
from jax.experimental import pallas as pl
from jax.experimental.pallas import tpu as pltpu
from jax.sharding import Mesh
from jax.sharding import PartitionSpec as P


SEQ = ("seq_0", "seq_1")
SEQ_0 = 8
BAT = 2

masked_score = -1e30
empty_score = -3e38
lanes = 128
terms = 3
small_grant = 8 * 2**20
large_grant = int(52.8 * 2**20)


def split_terms(value):
    parts = []
    for _ in range(terms):
        part = value.astype(jnp.bfloat16).astype(jnp.float32)
        parts.append(part)
        value = value - part
    return parts


def put_stats(stats, k, width, maxima, totals):
    lane = lax.broadcasted_iota(jnp.int32, stats.shape, 1)
    for i, part in enumerate(split_terms(maxima) + split_terms(totals)):
        stats = jnp.where(lane == i * width + k, part, stats)
    return stats


def take_stats(stats, width):
    parts = [stats[..., i * width : (i + 1) * width] for i in range(2 * terms)]
    return (parts[0] + parts[1] + parts[2], parts[3] + parts[4] + parts[5])


def prepare_kernel(lengths, queries, own_heads, limits):
    own, heads, _ = own_heads.shape
    side = lax.axis_index("bat")
    for i in range(own):
        own_heads[i] = queries[i, pl.ds(pl.multiple_of(side * heads, heads), heads), :]
        limits[i, :] = jnp.full((lanes,), lengths[side * own + i], jnp.int32)
        limits[own + i, :] = jnp.full((lanes,), lengths[(1 - side) * own + i], jnp.int32)


def prepare(lengths, queries, heads):
    vmem = pl.BlockSpec(memory_space=pltpu.VMEM)
    own, _, query_width = queries.shape
    return pl.pallas_call(
        prepare_kernel,
        out_shape=[
            jax.ShapeDtypeStruct((own, heads, query_width), queries.dtype),
            jax.ShapeDtypeStruct((BAT * own, lanes), jnp.int32),
        ],
        in_specs=[pl.BlockSpec(memory_space=pltpu.SMEM), vmem],
        out_specs=[vmem, vmem],
        compiler_params=pltpu.CompilerParams(vmem_limit_bytes=small_grant),
        cost_estimate=pl.CostEstimate(flops=10**7, bytes_accessed=10**5, transcendentals=0),
        name="prepare",
    )(lengths, queries)


def attend_kernel(
    scaling, own_heads, received, limits, cache, key, value, out,
    keys, up, values, heads_first, joined, scores, latent, arrived,
):
    own, heads, _ = own_heads.shape
    nope_width, latent_width = key.shape[1:]
    requests, _, shard_len = keys.shape
    side = lax.axis_index("bat")
    start = (lax.axis_index("seq_0") * lax.axis_size("seq_1") + lax.axis_index("seq_1")) * shard_len
    order = [side * own + i for i in range(own)] + [(1 - side) * own + i for i in range(own)]
    key_copy = pltpu.make_async_copy(key, up, arrived.at[requests])
    value_copy = pltpu.make_async_copy(value, values, arrived.at[requests + 1])
    copies = [
        pltpu.make_async_copy(cache.at[g], keys.at[i], arrived.at[i]) for i, g in enumerate(order)
    ]
    key_copy.start()
    for copy in copies:
        copy.start()
    value_copy.start()

    mine = pl.ds(pl.multiple_of(side * heads, heads), heads)
    rotary = []
    for i in range(requests):
        row = own_heads[i] if i < own else received[i - own, mine, :]
        heads_first[i] = row[:, :nope_width].astype(jnp.float32)
        rotary.append(row[:, nope_width:])
    key_copy.wait()
    for h in range(heads):
        joined[:, h, :] = jnp.dot(
            heads_first[:, h, :].astype(jnp.bfloat16), up[h], preferred_element_type=jnp.float32
        )
    lane = lax.broadcasted_iota(jnp.int32, (heads, shard_len), 1) + start
    for i in range(requests):
        copies[i].wait()
        part = jnp.dot(
            joined[i].astype(jnp.bfloat16), keys[i, :latent_width], preferred_element_type=jnp.float32
        )
        part += jnp.dot(rotary[i], keys[i, latent_width:], preferred_element_type=jnp.float32)
        scores[i] = jnp.where(lane < limits[i : i + 1, :1], part * scaling, masked_score)
    every = scores[...]
    maxima = jnp.max(every, axis=2, keepdims=True)
    weights = jnp.exp(every - maxima)
    totals = jnp.sum(weights, axis=2, keepdims=True)
    weights = weights.astype(jnp.bfloat16)
    for i in range(requests):
        latent[:, i, :] = lax.dot_general(
            weights[i],
            keys[i, :latent_width],
            (((1,), (1,)), ((), ())),
            preferred_element_type=jnp.float32,
        )
    value_copy.wait()
    for h in range(heads):
        heads_first[:, h, :] = jnp.dot(
            latent[h].astype(jnp.bfloat16), values[h], preferred_element_type=jnp.float32
        )
    for half in range(BAT):
        stats = jnp.zeros((heads, lanes), jnp.float32)
        for k in range(own):
            stats = put_stats(stats, k, own, maxima[half * own + k], totals[half * own + k])
        block = heads_first[half * own : (half + 1) * own].reshape(own * heads, lanes)
        block = jnp.concatenate([block, stats], axis=0).astype(jnp.bfloat16)
        target = side if half == 0 else 1 - side
        for x in range(out.shape[0]):
            out[x, target] = block


def attend(own_heads, received, limits, cache, key, value, copies):
    own, heads, query_width = own_heads.shape
    latent_width = key.shape[2]
    requests, shard_len, _ = cache.shape
    turned = jnp.swapaxes(cache, 1, 2)
    vmem, hbm = pl.BlockSpec(memory_space=pltpu.VMEM), pl.BlockSpec(memory_space=pltpu.HBM)
    return pl.pallas_call(
        functools.partial(attend_kernel, query_width ** (-0.5)),
        out_shape=jax.ShapeDtypeStruct((copies, BAT, (own + 1) * heads, lanes), jnp.bfloat16),
        in_specs=[vmem, vmem, vmem, hbm, hbm, hbm],
        out_specs=vmem,
        scratch_shapes=[
            pltpu.VMEM(turned.shape, turned.dtype),
            pltpu.VMEM(key.shape, key.dtype),
            pltpu.VMEM(value.shape, value.dtype),
            pltpu.VMEM((requests, heads, lanes), jnp.float32),
            pltpu.VMEM((requests, heads, latent_width), jnp.float32),
            pltpu.VMEM((requests, heads, shard_len), jnp.float32),
            pltpu.VMEM((heads, requests, latent_width), jnp.float32),
            pltpu.SemaphoreType.DMA((requests + 2,)),
        ],
        compiler_params=pltpu.CompilerParams(vmem_limit_bytes=large_grant),
        name="attend",
    )(own_heads, received, limits, turned, key, value)


def merged(tiles, stats, width):
    heads = stats.shape[1]
    maxima, totals = take_stats(stats, width)
    maxima = jnp.where(totals > 0, maxima, empty_score)
    highest = jnp.max(maxima, axis=0, keepdims=True)
    factors = jnp.exp(maxima - highest)
    total = jnp.sum(totals * factors, axis=0)
    sums = []
    for k in range(width):
        part = tiles[:, k * heads : (k + 1) * heads] * factors[:, :, k : k + 1]
        sums.append(jnp.sum(part, axis=0))
    return sums, highest[0], total


def summed(heads, pieces):
    width = pieces.shape[1] // heads - 1
    block = pieces.astype(jnp.float32)
    return merged(block[:, : width * heads], block[:, width * heads :], width)


def packed(heads, sums, highest, total):
    stats = jnp.zeros((heads, lanes), jnp.float32)
    for k in range(len(sums)):
        stats = put_stats(stats, k, len(sums), highest[:, k : k + 1], total[:, k : k + 1])
    return jnp.concatenate([*sums, stats], axis=0).astype(jnp.bfloat16)


def merge_across_kernel(heads, pieces, out, plane):
    plane[0] = lax.axis_index("seq_1")
    for b in range(BAT):
        out[b] = packed(heads, *summed(heads, pieces[:, b]))


def merged_across(heads, pieces):
    vmem, smem = pl.BlockSpec(memory_space=pltpu.VMEM), pl.BlockSpec(memory_space=pltpu.SMEM)
    partial, plane = pl.pallas_call(
        functools.partial(merge_across_kernel, heads),
        out_shape=[
            jax.ShapeDtypeStruct(pieces.shape[1:], pieces.dtype),
            jax.ShapeDtypeStruct((1,), jnp.int32),
        ],
        in_specs=[vmem],
        out_specs=[vmem, smem],
        compiler_params=pltpu.CompilerParams(vmem_limit_bytes=small_grant),
        name="merge_across",
    )(pieces)
    return partial, plane[0]


def merge_kernel(heads, *refs):
    *parts, out = refs
    for b in range(BAT):
        out[b] = packed(heads, *summed(heads, jnp.stack([part[b] for part in parts])))


def finish_kernel(heads, *refs):
    *parts, out = refs
    for b in range(BAT):
        sums, _, total = summed(heads, jnp.stack([part[b] for part in parts]))
        for k in range(len(sums)):
            out[k, b] = (sums[k] / total[:, k : k + 1]).astype(jnp.bfloat16)


def whole(kernel, heads, shape, name, *operands):
    vmem = pl.BlockSpec(memory_space=pltpu.VMEM)
    return pl.pallas_call(
        functools.partial(kernel, heads),
        out_shape=jax.ShapeDtypeStruct(shape, jnp.bfloat16),
        in_specs=[vmem] * len(operands),
        out_specs=vmem,
        compiler_params=pltpu.CompilerParams(vmem_limit_bytes=small_grant),
        name=name,
    )(*operands)


def moved(value, pairs):
    return lax.ppermute(value, "seq_1", pairs)


def one_of(plane, planes):
    return functools.reduce(jnp.logical_or, [plane == p for p in planes])


def within(plane, planes, step, value):
    return lax.cond(one_of(plane, planes), step, lambda kept: kept, value)


def gathered_at_first(plane, last, partial, heads, shape):
    merge = functools.partial(whole, merge_kernel, heads, partial.shape, "merge")

    def folded(pairs):
        return lambda kept: merge(kept, moved(kept, pairs))

    def tree(kept):
        kept = within(plane, range(2, 10), folded([(9, 8), (7, 6), (5, 4), (3, 2)]), kept)
        kept = within(plane, (4, 6), folded([(6, 4)]), kept)
        kept = within(plane, (2, 4), folded([(4, 2)]), kept)
        sources = [2, 8, *range(10, last - 2)]

        def collect(kept):
            return merge(kept, *[moved(kept, [(p, 1)]) for p in sources])

        return within(plane, (1, *sources), collect, kept)

    partial = within(plane, range(1, last - 2), tree, partial)

    def finish(kept):
        parts = [moved(kept, [(p, 0)]) for p in (last - 2, last - 1, 1, last)]
        return whole(finish_kernel, heads, shape, "finish", kept, *parts)

    planes = (0, 1, last - 2, last - 1, last)

    def unfinished(kept):
        return kept[:, : shape[0] * heads].reshape(shape)

    return lax.cond(one_of(plane, planes), finish, unfinished, partial)


def handed_on(plane, result):
    rounds = (
        ([(0, 1)],),
        ([(1, 2)],),
        ([(2, 4)], [(2, 3)]),
        ([(3, 5), (4, 7)], [(3, 6), (4, 8)]),
        ([(5, 9), (6, 11), (7, 13), (8, 15)], [(5, 10), (6, 12), (7, 14)]),
    )
    for moves in rounds:

        def step(kept, moves=moves):
            arrived = [moved(kept, pairs) for pairs in moves]
            for value, pairs in zip(arrived, moves):
                kept = jnp.where(one_of(plane, [target for _, target in pairs]), value, kept)
            return kept

        planes = sorted({p for pairs in moves for pair in pairs for p in pair})
        result = within(plane, planes, step, result)
    return result


def per_device(queries, latent_cache, cache_lengths, key_weight, value_weight):
    heads = key_weight.shape[0]
    received = lax.ppermute(queries, "bat", [(0, 1), (1, 0)])
    own_heads, limits = prepare(cache_lengths, queries, heads)
    across, along = lax.axis_size("seq_0"), lax.axis_size("seq_1")
    partial = attend(
        own_heads, received, limits, latent_cache, key_weight, value_weight, across
    )
    shape = partial.shape
    pieces = lax.all_to_all(
        partial.reshape(across * BAT, *shape[2:]), ("seq_0", "bat"), 0, 0, tiled=True
    ).reshape(shape)
    partial, plane = merged_across(heads, pieces)
    own, value_width = queries.shape[0], value_weight.shape[2]
    result = gathered_at_first(plane, along - 1, partial, heads, (own, BAT, heads, value_width))
    result = handed_on(plane, result)
    return result.reshape(own, BAT * heads, value_width)


def solution(mesh):
    torus = Mesh(
        mesh.devices.reshape(mesh.shape["grp"], SEQ_0, mesh.shape["seq"] // SEQ_0, mesh.shape["bat"]),
        ("grp", "seq_0", "seq_1", "bat"),
    )
    placed = (
        P(("grp", "bat"), None, None),
        P("grp", SEQ, None),
        P("grp"),
        P("bat", None, None),
        P("bat", None, None),
    )
    return jax.shard_map(
        per_device,
        mesh=torus,
        in_specs=placed,
        out_specs=P(("grp", "bat"), None, None),
        check_vma=False,
    )
```

```python
import functools

import jax
import jax.numpy as jnp
from jax import lax
from jax.experimental import pallas as pl
from jax.experimental.pallas import tpu as pltpu
from jax.sharding import Mesh
from jax.sharding import PartitionSpec as P


SEQ = ("seq_0", "seq_1")
SEQ_0 = 8
BAT = 2

masked_score = -1e30
empty_score = -3e38
lanes = 128
terms = 3
small_grant = 8 * 2**20
large_grant = int(52.8 * 2**20)


def split_terms(value):
    parts = []
    for _ in range(terms):
        part = value.astype(jnp.bfloat16).astype(jnp.float32)
        parts.append(part)
        value = value - part
    return parts


def put_stats(stats, k, width, maxima, totals):
    lane = lax.broadcasted_iota(jnp.int32, stats.shape, 1)
    for i, part in enumerate(split_terms(maxima) + split_terms(totals)):
        stats = jnp.where(lane == i * width + k, part, stats)
    return stats


def take_stats(stats, width):
    parts = [stats[..., i * width : (i + 1) * width] for i in range(2 * terms)]
    return (parts[0] + parts[1] + parts[2], parts[3] + parts[4] + parts[5])


def prepare_kernel(lengths, queries, *refs):
    *_, own_heads, limits = refs
    own, heads, _ = own_heads.shape
    side = lax.axis_index("bat")
    for i in range(own):
        own_heads[i] = queries[i, pl.ds(pl.multiple_of(side * heads, heads), heads), :]
        limits[i, :] = jnp.full((lanes,), lengths[side * own + i], jnp.int32)
        limits[own + i, :] = jnp.full((lanes,), lengths[(1 - side) * own + i], jnp.int32)


def prepare(lengths, queries, heads, *first):
    vmem, smem = pl.BlockSpec(memory_space=pltpu.VMEM), pl.BlockSpec(memory_space=pltpu.SMEM)
    own, _, query_width = queries.shape
    return pl.pallas_call(
        prepare_kernel,
        out_shape=[
            jax.ShapeDtypeStruct((own, heads, query_width), queries.dtype),
            jax.ShapeDtypeStruct((BAT * own, lanes), jnp.int32),
        ],
        in_specs=[smem, vmem, *[smem] * len(first)],
        out_specs=[vmem, vmem],
        compiler_params=pltpu.CompilerParams(vmem_limit_bytes=small_grant),
        cost_estimate=pl.CostEstimate(flops=10**7, bytes_accessed=10**5, transcendentals=0),
        name="prepare",
    )(lengths, queries, *[value.astype(jnp.int32).reshape(1) for value in first])


def attend_kernel(
    scaling, own_heads, received, limits, cache, key, value, out,
    keys, up, values, heads_first, joined, scores, latent, arrived,
):
    own, heads, _ = own_heads.shape
    nope_width, latent_width = key.shape[1:]
    requests, _, shard_len = keys.shape
    side = lax.axis_index("bat")
    start = (lax.axis_index("seq_0") * lax.axis_size("seq_1") + lax.axis_index("seq_1")) * shard_len
    order = [side * own + i for i in range(own)] + [(1 - side) * own + i for i in range(own)]
    key_copy = pltpu.make_async_copy(key, up, arrived.at[requests])
    value_copy = pltpu.make_async_copy(value, values, arrived.at[requests + 1])
    copies = [
        pltpu.make_async_copy(cache.at[g], keys.at[i], arrived.at[i]) for i, g in enumerate(order)
    ]
    key_copy.start()
    for copy in copies:
        copy.start()
    value_copy.start()

    mine = pl.ds(pl.multiple_of(side * heads, heads), heads)
    rotary = []
    for i in range(requests):
        row = own_heads[i] if i < own else received[i - own, mine, :]
        heads_first[i] = row[:, :nope_width].astype(jnp.float32)
        rotary.append(row[:, nope_width:])
    key_copy.wait()
    for h in range(heads):
        joined[:, h, :] = jnp.dot(
            heads_first[:, h, :].astype(jnp.bfloat16), up[h], preferred_element_type=jnp.float32
        )
    lane = lax.broadcasted_iota(jnp.int32, (heads, shard_len), 1) + start
    for i in range(requests):
        copies[i].wait()
        part = jnp.dot(
            joined[i].astype(jnp.bfloat16), keys[i, :latent_width], preferred_element_type=jnp.float32
        )
        part += jnp.dot(rotary[i], keys[i, latent_width:], preferred_element_type=jnp.float32)
        scores[i] = jnp.where(lane < limits[i : i + 1, :1], part * scaling, masked_score)
    every = scores[...]
    maxima = jnp.max(every, axis=2, keepdims=True)
    weights = jnp.exp(every - maxima)
    totals = jnp.sum(weights, axis=2, keepdims=True)
    weights = weights.astype(jnp.bfloat16)
    for i in range(requests):
        latent[:, i, :] = lax.dot_general(
            weights[i],
            keys[i, :latent_width],
            (((1,), (1,)), ((), ())),
            preferred_element_type=jnp.float32,
        )
    value_copy.wait()
    for h in range(heads):
        heads_first[:, h, :] = jnp.dot(
            latent[h].astype(jnp.bfloat16), values[h], preferred_element_type=jnp.float32
        )
    for half in range(BAT):
        stats = jnp.zeros((heads, lanes), jnp.float32)
        for k in range(own):
            stats = put_stats(stats, k, own, maxima[half * own + k], totals[half * own + k])
        block = heads_first[half * own : (half + 1) * own].reshape(own * heads, lanes)
        block = jnp.concatenate([block, stats], axis=0).astype(jnp.bfloat16)
        target = side if half == 0 else 1 - side
        for x in range(out.shape[0]):
            out[x, target] = block


def attend(own_heads, received, limits, cache, key, value, copies):
    own, heads, query_width = own_heads.shape
    latent_width = key.shape[2]
    requests, shard_len, _ = cache.shape
    turned = jnp.swapaxes(cache, 1, 2)
    vmem, hbm = pl.BlockSpec(memory_space=pltpu.VMEM), pl.BlockSpec(memory_space=pltpu.HBM)
    return pl.pallas_call(
        functools.partial(attend_kernel, query_width ** (-0.5)),
        out_shape=jax.ShapeDtypeStruct((copies, BAT, (own + 1) * heads, lanes), jnp.bfloat16),
        in_specs=[vmem, vmem, vmem, hbm, hbm, hbm],
        out_specs=vmem,
        scratch_shapes=[
            pltpu.VMEM(turned.shape, turned.dtype),
            pltpu.VMEM(key.shape, key.dtype),
            pltpu.VMEM(value.shape, value.dtype),
            pltpu.VMEM((requests, heads, lanes), jnp.float32),
            pltpu.VMEM((requests, heads, latent_width), jnp.float32),
            pltpu.VMEM((requests, heads, shard_len), jnp.float32),
            pltpu.VMEM((heads, requests, latent_width), jnp.float32),
            pltpu.SemaphoreType.DMA((requests + 2,)),
        ],
        compiler_params=pltpu.CompilerParams(vmem_limit_bytes=large_grant),
        name="attend",
    )(own_heads, received, limits, turned, key, value)


def merged(tiles, stats, width):
    heads = stats.shape[1]
    maxima, totals = take_stats(stats, width)
    maxima = jnp.where(totals > 0, maxima, empty_score)
    highest = jnp.max(maxima, axis=0, keepdims=True)
    factors = jnp.exp(maxima - highest)
    total = jnp.sum(totals * factors, axis=0)
    sums = []
    for k in range(width):
        part = tiles[:, k * heads : (k + 1) * heads] * factors[:, :, k : k + 1]
        sums.append(jnp.sum(part, axis=0))
    return sums, highest[0], total


def summed(heads, pieces):
    width = pieces.shape[1] // heads - 1
    block = pieces.astype(jnp.float32)
    return merged(block[:, : width * heads], block[:, width * heads :], width)


def packed(heads, sums, highest, total):
    stats = jnp.zeros((heads, lanes), jnp.float32)
    for k in range(len(sums)):
        stats = put_stats(stats, k, len(sums), highest[:, k : k + 1], total[:, k : k + 1])
    return jnp.concatenate([*sums, stats], axis=0).astype(jnp.bfloat16)


def merge_across_kernel(heads, pieces, out):
    for b in range(BAT):
        out[b] = packed(heads, *summed(heads, pieces[:, b]))


def merge_kernel(heads, *refs):
    *parts, out = refs
    for b in range(BAT):
        out[b] = packed(heads, *summed(heads, jnp.stack([part[b] for part in parts])))


def finish_kernel(heads, *refs):
    *parts, out = refs
    first = lax.axis_index("seq_1") == 0
    for b in range(BAT):
        sums, _, total = summed(heads, jnp.stack([part[b] for part in parts]))
        for k in range(len(sums)):
            result = sums[k] / total[:, k : k + 1]
            out[k, b] = jnp.where(first, result, 0.0).astype(jnp.bfloat16)


def whole(kernel, heads, shape, name, *operands):
    vmem = pl.BlockSpec(memory_space=pltpu.VMEM)
    return pl.pallas_call(
        functools.partial(kernel, heads),
        out_shape=jax.ShapeDtypeStruct(shape, jnp.bfloat16),
        in_specs=[vmem] * len(operands),
        out_specs=vmem,
        compiler_params=pltpu.CompilerParams(vmem_limit_bytes=small_grant),
        name=name,
    )(*operands)


def moved(value, pairs):
    return lax.ppermute(value, "seq_1", pairs)


def one_of(plane, planes):
    return functools.reduce(jnp.logical_or, [plane == p for p in planes])


def within(inside, step, value):
    return lax.cond(inside, step, lambda kept: kept, value)


folds = (
    [[(9, 8), (7, 6), (5, 4), (3, 2)]],
    [[(6, 4)]],
    [[(4, 2)]],
    [[(2, 1)], [(8, 1)], [(10, 1)], [(11, 1)], [(12, 1)]],
)
last_fold = [[(13, 0)], [(14, 0)], [(1, 0)], [(15, 0)]]
rounds = (
    [[(0, 1)]],
    [[(1, 2)]],
    [[(2, 4)], [(2, 3)]],
    [[(3, 5), (4, 7)], [(3, 6), (4, 8)]],
    [[(5, 9), (6, 11), (7, 13), (8, 15)], [(5, 10), (6, 12), (7, 14)]],
)


def takes_part(moves):
    planes = sorted({p for pairs in moves for pair in pairs for p in pair})
    return one_of(lax.axis_index("seq_1"), planes)


def gathered_at_first(inside, partial, heads, shape):
    def fold(moves, kept):
        parts = [moved(kept, pairs) for pairs in moves]
        return whole(merge_kernel, heads, kept.shape, "merge", kept, *parts)

    def finish(kept):
        parts = [moved(kept, pairs) for pairs in last_fold]
        return whole(finish_kernel, heads, shape, "finish", kept, *parts)

    def unfinished(kept):
        return kept[:, : shape[0] * heads].reshape(shape) * 0

    for moves, here in zip(folds, inside):
        partial = within(here, functools.partial(fold, moves), partial)
    return lax.cond(inside[-1], finish, unfinished, partial)


def handed_on(inside, result):
    def step(moves, kept):
        return functools.reduce(jnp.add, [moved(kept, pairs) for pairs in moves], kept)

    for moves, here in zip(rounds, inside):
        result = within(here, functools.partial(step, moves), result)
    return result


def per_device(queries, latent_cache, cache_lengths, key_weight, value_weight):
    heads = key_weight.shape[0]
    received = lax.ppermute(queries, "bat", [(0, 1), (1, 0)])
    to_first = [takes_part(moves) for moves in (*folds, last_fold)]
    from_first = [takes_part(moves) for moves in rounds]
    own_heads, limits = prepare(cache_lengths, queries, heads, *to_first, *from_first)
    across = lax.axis_size("seq_0")
    partial = attend(
        own_heads, received, limits, latent_cache, key_weight, value_weight, across
    )
    shape = partial.shape
    pieces = lax.all_to_all(
        partial.reshape(across * BAT, *shape[2:]), ("seq_0", "bat"), 0, 0, tiled=True
    ).reshape(shape)
    partial = whole(merge_across_kernel, heads, shape[1:], "merge_across", pieces)
    own, value_width = queries.shape[0], value_weight.shape[2]
    shape = (own, BAT, heads, value_width)
    result = gathered_at_first(to_first, partial, heads, shape)
    result = handed_on(from_first, result)
    return result.reshape(own, BAT * heads, value_width)


def solution(mesh):
    torus = Mesh(
        mesh.devices.reshape(mesh.shape["grp"], SEQ_0, mesh.shape["seq"] // SEQ_0, mesh.shape["bat"]),
        ("grp", "seq_0", "seq_1", "bat"),
    )
    placed = (
        P(("grp", "bat"), None, None),
        P("grp", SEQ, None),
        P("grp"),
        P("bat", None, None),
        P("bat", None, None),
    )
    return jax.shard_map(
        per_device,
        mesh=torus,
        in_specs=placed,
        out_specs=P(("grp", "bat"), None, None),
        check_vma=False,
    )
```

```python
import functools

import jax
import jax.numpy as jnp
from jax import lax
from jax.experimental import pallas as pl
from jax.experimental.pallas import tpu as pltpu
from jax.sharding import Mesh
from jax.sharding import PartitionSpec as P


SEQ = ("seq_0", "seq_1")
SEQ_0 = 8
BAT = 2

masked_score = -1e30
empty_score = -3e38
lanes = 128
terms = 3
small_grant = 8 * 2**20
large_grant = int(52.8 * 2**20)


def split_terms(value):
    parts = []
    for _ in range(terms):
        part = value.astype(jnp.bfloat16).astype(jnp.float32)
        parts.append(part)
        value = value - part
    return parts


def put_stats(stats, k, width, maxima, totals):
    lane = lax.broadcasted_iota(jnp.int32, stats.shape, 1)
    for i, part in enumerate(split_terms(maxima) + split_terms(totals)):
        stats = jnp.where(lane == i * width + k, part, stats)
    return stats


def take_stats(stats, width):
    parts = [stats[..., i * width : (i + 1) * width] for i in range(2 * terms)]
    return (parts[0] + parts[1] + parts[2], parts[3] + parts[4] + parts[5])


def prepare_kernel(lengths, queries, *refs):
    *_, own_heads, limits = refs
    own, heads, _ = own_heads.shape
    side = lax.axis_index("bat")
    for i in range(own):
        own_heads[i] = queries[i, pl.ds(pl.multiple_of(side * heads, heads), heads), :]
        limits[i, :] = jnp.full((lanes,), lengths[side * own + i], jnp.int32)
        limits[own + i, :] = jnp.full((lanes,), lengths[(1 - side) * own + i], jnp.int32)


def prepare(lengths, queries, heads, *first):
    vmem, smem = pl.BlockSpec(memory_space=pltpu.VMEM), pl.BlockSpec(memory_space=pltpu.SMEM)
    own, _, query_width = queries.shape
    return pl.pallas_call(
        prepare_kernel,
        out_shape=[
            jax.ShapeDtypeStruct((own, heads, query_width), queries.dtype),
            jax.ShapeDtypeStruct((BAT * own, lanes), jnp.int32),
        ],
        in_specs=[smem, vmem, *[smem] * len(first)],
        out_specs=[vmem, vmem],
        compiler_params=pltpu.CompilerParams(vmem_limit_bytes=small_grant),
        cost_estimate=pl.CostEstimate(flops=10**7, bytes_accessed=10**5, transcendentals=0),
        name="prepare",
    )(lengths, queries, *[value.astype(jnp.int32).reshape(1) for value in first])


def attend_kernel(
    scaling, own_heads, received, limits, cache, key, value, out,
    keys, up, values, heads_first, joined, scores, latent, arrived,
):
    own, heads, _ = own_heads.shape
    nope_width, latent_width = key.shape[1:]
    requests, _, shard_len = keys.shape
    side = lax.axis_index("bat")
    start = (lax.axis_index("seq_0") * lax.axis_size("seq_1") + lax.axis_index("seq_1")) * shard_len
    order = [side * own + i for i in range(own)] + [(1 - side) * own + i for i in range(own)]
    key_copy = pltpu.make_async_copy(key, up, arrived.at[requests])
    value_copy = pltpu.make_async_copy(value, values, arrived.at[requests + 1])
    copies = [
        pltpu.make_async_copy(cache.at[g], keys.at[i], arrived.at[i]) for i, g in enumerate(order)
    ]
    key_copy.start()
    for copy in copies:
        copy.start()
    value_copy.start()

    mine = pl.ds(pl.multiple_of(side * heads, heads), heads)
    rotary = []
    for i in range(requests):
        row = own_heads[i] if i < own else received[i - own, mine, :]
        heads_first[i] = row[:, :nope_width].astype(jnp.float32)
        rotary.append(row[:, nope_width:])
    key_copy.wait()
    for h in range(heads):
        joined[:, h, :] = jnp.dot(
            heads_first[:, h, :].astype(jnp.bfloat16), up[h], preferred_element_type=jnp.float32
        )
    lane = lax.broadcasted_iota(jnp.int32, (heads, shard_len), 1) + start
    maxima, totals = [], []
    for half in range(0, requests, own):
        rows = range(half, half + own)
        for i in rows:
            copies[i].wait()
            part = jnp.dot(
                joined[i].astype(jnp.bfloat16),
                keys[i, :latent_width],
                preferred_element_type=jnp.float32,
            )
            part += jnp.dot(rotary[i], keys[i, latent_width:], preferred_element_type=jnp.float32)
            scores[i] = jnp.where(lane < limits[i : i + 1, :1], part * scaling, masked_score)
        every = scores[half : half + own]
        highest = jnp.max(every, axis=2, keepdims=True)
        weights = jnp.exp(every - highest)
        maxima.append(highest)
        totals.append(jnp.sum(weights, axis=2, keepdims=True))
        weights = weights.astype(jnp.bfloat16)
        for i in rows:
            latent[:, i, :] = lax.dot_general(
                weights[i - half],
                keys[i, :latent_width],
                (((1,), (1,)), ((), ())),
                preferred_element_type=jnp.float32,
            )
    value_copy.wait()
    for h in range(heads):
        heads_first[:, h, :] = jnp.dot(
            latent[h].astype(jnp.bfloat16), values[h], preferred_element_type=jnp.float32
        )
    for half in range(BAT):
        stats = jnp.zeros((heads, lanes), jnp.float32)
        for k in range(own):
            stats = put_stats(stats, k, own, maxima[half][k], totals[half][k])
        block = heads_first[half * own : (half + 1) * own].reshape(own * heads, lanes)
        block = jnp.concatenate([block, stats], axis=0).astype(jnp.bfloat16)
        target = side if half == 0 else 1 - side
        for x in range(out.shape[0]):
            out[x, target] = block


def attend(own_heads, received, limits, cache, key, value, copies):
    own, heads, query_width = own_heads.shape
    latent_width = key.shape[2]
    requests, shard_len, _ = cache.shape
    turned = jnp.swapaxes(cache, 1, 2)
    vmem, hbm = pl.BlockSpec(memory_space=pltpu.VMEM), pl.BlockSpec(memory_space=pltpu.HBM)
    return pl.pallas_call(
        functools.partial(attend_kernel, query_width ** (-0.5)),
        out_shape=jax.ShapeDtypeStruct((copies, BAT, (own + 1) * heads, lanes), jnp.bfloat16),
        in_specs=[vmem, vmem, vmem, hbm, hbm, hbm],
        out_specs=vmem,
        scratch_shapes=[
            pltpu.VMEM(turned.shape, turned.dtype),
            pltpu.VMEM(key.shape, key.dtype),
            pltpu.VMEM(value.shape, value.dtype),
            pltpu.VMEM((requests, heads, lanes), jnp.float32),
            pltpu.VMEM((requests, heads, latent_width), jnp.float32),
            pltpu.VMEM((requests, heads, shard_len), jnp.float32),
            pltpu.VMEM((heads, requests, latent_width), jnp.float32),
            pltpu.SemaphoreType.DMA((requests + 2,)),
        ],
        compiler_params=pltpu.CompilerParams(vmem_limit_bytes=large_grant),
        name="attend",
    )(own_heads, received, limits, turned, key, value)


def merged(tiles, stats, width):
    heads = stats.shape[1]
    maxima, totals = take_stats(stats, width)
    maxima = jnp.where(totals > 0, maxima, empty_score)
    highest = jnp.max(maxima, axis=0, keepdims=True)
    factors = jnp.exp(maxima - highest)
    total = jnp.sum(totals * factors, axis=0)
    sums = []
    for k in range(width):
        part = tiles[:, k * heads : (k + 1) * heads] * factors[:, :, k : k + 1]
        sums.append(jnp.sum(part, axis=0))
    return sums, highest[0], total


def summed(heads, pieces):
    width = pieces.shape[1] // heads - 1
    block = pieces.astype(jnp.float32)
    return merged(block[:, : width * heads], block[:, width * heads :], width)


def packed(heads, sums, highest, total):
    stats = jnp.zeros((heads, lanes), jnp.float32)
    for k in range(len(sums)):
        stats = put_stats(stats, k, len(sums), highest[:, k : k + 1], total[:, k : k + 1])
    return jnp.concatenate([*sums, stats], axis=0).astype(jnp.bfloat16)


def merge_across_kernel(heads, pieces, out):
    for b in range(BAT):
        out[b] = packed(heads, *summed(heads, pieces[:, b]))


def finish_kernel(heads, *refs):
    *parts, out = refs
    here = lax.axis_index("seq_1") == root
    for b in range(BAT):
        sums, _, total = summed(heads, jnp.stack([part[b] for part in parts]))
        for k in range(len(sums)):
            result = sums[k] / total[:, k : k + 1]
            out[k, b] = jnp.where(here, result, 0.0).astype(jnp.bfloat16)


def whole(kernel, heads, shape, name, *operands):
    vmem = pl.BlockSpec(memory_space=pltpu.VMEM)
    return pl.pallas_call(
        functools.partial(kernel, heads),
        out_shape=jax.ShapeDtypeStruct(shape, jnp.bfloat16),
        in_specs=[vmem] * len(operands),
        out_specs=vmem,
        compiler_params=pltpu.CompilerParams(vmem_limit_bytes=small_grant),
        name=name,
    )(*operands)


def moved(value, pairs):
    return lax.ppermute(value, "seq_1", pairs)


def one_of(plane, planes):
    return functools.reduce(jnp.logical_or, [plane == p for p in planes])


def within(inside, step, value):
    return lax.cond(inside, step, lambda kept: kept, value)


root = 1
sources = (*range(2, 14), 0, 14, 15)
rounds = (
    [[(1, 3)], [(1, 2)], [(1, 0)]],
    [[(2, 5), (3, 7)], [(2, 4), (3, 6)]],
    [[(4, 9), (5, 11), (6, 13), (7, 15)], [(4, 8), (5, 10), (6, 12), (7, 14)]],
)


def takes_part(moves):
    planes = sorted({p for pairs in moves for pair in pairs for p in pair})
    return one_of(lax.axis_index("seq_1"), planes)


def gathered_at_root(partial, heads, shape):
    parts = [moved(partial, [(p, root)]) for p in sources]
    return whole(finish_kernel, heads, shape, "finish", partial, *parts)


def handed_on(inside, result):
    def step(moves, kept):
        return functools.reduce(jnp.add, [moved(kept, pairs) for pairs in moves], kept)

    for moves, here in zip(rounds, inside):
        result = within(here, functools.partial(step, moves), result)
    return result


def per_device(queries, latent_cache, cache_lengths, key_weight, value_weight):
    heads = key_weight.shape[0]
    received = lax.ppermute(queries, "bat", [(0, 1), (1, 0)])
    in_rounds = [takes_part(moves) for moves in rounds]
    own_heads, limits = prepare(cache_lengths, queries, heads, *in_rounds)
    across = lax.axis_size("seq_0")
    partial = attend(
        own_heads, received, limits, latent_cache, key_weight, value_weight, across
    )
    shape = partial.shape
    pieces = lax.all_to_all(
        partial.reshape(across * BAT, *shape[2:]), ("seq_0", "bat"), 0, 0, tiled=True
    ).reshape(shape)
    partial = whole(merge_across_kernel, heads, shape[1:], "merge_across", pieces)
    own, value_width = queries.shape[0], value_weight.shape[2]
    shape = (own, BAT, heads, value_width)
    result = gathered_at_root(partial, heads, shape)
    result = handed_on(in_rounds, result)
    return result.reshape(own, BAT * heads, value_width)


def solution(mesh):
    torus = Mesh(
        mesh.devices.reshape(mesh.shape["grp"], SEQ_0, mesh.shape["seq"] // SEQ_0, mesh.shape["bat"]),
        ("grp", "seq_0", "seq_1", "bat"),
    )
    placed = (
        P(("grp", "bat"), None, None),
        P("grp", SEQ, None),
        P("grp"),
        P("bat", None, None),
        P("bat", None, None),
    )
    return jax.shard_map(
        per_device,
        mesh=torus,
        in_specs=placed,
        out_specs=P(("grp", "bat"), None, None),
        check_vma=False,
    )
```

```python
import functools

import jax
import jax.numpy as jnp
from jax import lax
from jax.experimental import pallas as pl
from jax.experimental.pallas import tpu as pltpu
from jax.sharding import Mesh
from jax.sharding import PartitionSpec as P


SEQ = ("seq_0", "seq_1")
SEQ_0 = 8
BAT = 2

masked_score = -1e30
empty_score = -3e38
lanes = 128
terms = 3
small_grant = 8 * 2**20
large_grant = int(52.8 * 2**20)


def split_terms(value):
    parts = []
    for _ in range(terms):
        part = value.astype(jnp.bfloat16).astype(jnp.float32)
        parts.append(part)
        value = value - part
    return parts


def put_stats(stats, k, width, maxima, totals):
    lane = lax.broadcasted_iota(jnp.int32, stats.shape, 1)
    for i, part in enumerate(split_terms(maxima) + split_terms(totals)):
        stats = jnp.where(lane == i * width + k, part, stats)
    return stats


def take_stats(stats, width):
    parts = [stats[..., i * width : (i + 1) * width] for i in range(2 * terms)]
    return (parts[0] + parts[1] + parts[2], parts[3] + parts[4] + parts[5])


def prepare_kernel(lengths, queries, *refs):
    *_, own_heads, limits = refs
    own, heads, _ = own_heads.shape
    side = lax.axis_index("bat")
    for i in range(own):
        own_heads[i] = queries[i, pl.ds(pl.multiple_of(side * heads, heads), heads), :]
        limits[i, :] = jnp.full((lanes,), lengths[side * own + i], jnp.int32)
        limits[own + i, :] = jnp.full((lanes,), lengths[(1 - side) * own + i], jnp.int32)


def prepare(lengths, queries, heads, *first):
    vmem, smem = pl.BlockSpec(memory_space=pltpu.VMEM), pl.BlockSpec(memory_space=pltpu.SMEM)
    own, _, query_width = queries.shape
    return pl.pallas_call(
        prepare_kernel,
        out_shape=[
            jax.ShapeDtypeStruct((own, heads, query_width), queries.dtype),
            jax.ShapeDtypeStruct((BAT * own, lanes), jnp.int32),
        ],
        in_specs=[smem, vmem, *[smem] * len(first)],
        out_specs=[vmem, vmem],
        compiler_params=pltpu.CompilerParams(vmem_limit_bytes=small_grant),
        cost_estimate=pl.CostEstimate(flops=10**7, bytes_accessed=10**5, transcendentals=0),
        name="prepare",
    )(lengths, queries, *[value.astype(jnp.int32).reshape(1) for value in first])


def attend_kernel(
    scaling, own_heads, received, limits, cache, key, value, out,
    keys, up, values, heads_first, joined, scores, latent, arrived,
):
    own, heads, _ = own_heads.shape
    nope_width, latent_width = key.shape[1:]
    requests, _, shard_len = keys.shape
    side = lax.axis_index("bat")
    start = (lax.axis_index("seq_0") * lax.axis_size("seq_1") + lax.axis_index("seq_1")) * shard_len
    order = [side * own + i for i in range(own)] + [(1 - side) * own + i for i in range(own)]
    key_copy = pltpu.make_async_copy(key, up, arrived.at[requests])
    value_copy = pltpu.make_async_copy(value, values, arrived.at[requests + 1])
    copies = [
        pltpu.make_async_copy(cache.at[g], keys.at[i], arrived.at[i]) for i, g in enumerate(order)
    ]
    key_copy.start()
    for copy in copies:
        copy.start()
    value_copy.start()

    mine = pl.ds(pl.multiple_of(side * heads, heads), heads)
    rotary = []
    for i in range(requests):
        row = own_heads[i] if i < own else received[i - own, mine, :]
        heads_first[i] = row[:, :nope_width].astype(jnp.float32)
        rotary.append(row[:, nope_width:])
    key_copy.wait()
    for h in range(heads):
        joined[:, h, :] = jnp.dot(
            heads_first[:, h, :].astype(jnp.bfloat16), up[h], preferred_element_type=jnp.float32
        )
    lane = lax.broadcasted_iota(jnp.int32, (heads, shard_len), 1) + start
    maxima, totals = [], []
    for half in range(0, requests, own):
        rows = range(half, half + own)
        for i in rows:
            copies[i].wait()
            part = jnp.dot(
                joined[i].astype(jnp.bfloat16),
                keys[i, :latent_width],
                preferred_element_type=jnp.float32,
            )
            part += jnp.dot(rotary[i], keys[i, latent_width:], preferred_element_type=jnp.float32)
            scores[i] = jnp.where(lane < limits[i : i + 1, :1], part * scaling, masked_score)
        every = scores[half : half + own]
        highest = jnp.max(every, axis=2, keepdims=True)
        weights = jnp.exp(every - highest)
        maxima.append(highest)
        totals.append(jnp.sum(weights, axis=2, keepdims=True))
        weights = weights.astype(jnp.bfloat16)
        for i in rows:
            latent[:, i, :] = lax.dot_general(
                weights[i - half],
                keys[i, :latent_width],
                (((1,), (1,)), ((), ())),
                preferred_element_type=jnp.float32,
            )
    value_copy.wait()
    for h in range(heads):
        heads_first[:, h, :] = jnp.dot(
            latent[h].astype(jnp.bfloat16), values[h], preferred_element_type=jnp.float32
        )
    for half in range(BAT):
        stats = jnp.zeros((heads, lanes), jnp.float32)
        for k in range(own):
            stats = put_stats(stats, k, own, maxima[half][k], totals[half][k])
        block = heads_first[half * own : (half + 1) * own].reshape(own * heads, lanes)
        block = jnp.concatenate([block, stats], axis=0).astype(jnp.bfloat16)
        target = side if half == 0 else 1 - side
        for x in range(out.shape[0]):
            out[x, target] = block


def attend(own_heads, received, limits, cache, key, value, copies):
    own, heads, query_width = own_heads.shape
    latent_width = key.shape[2]
    requests, shard_len, _ = cache.shape
    turned = jnp.swapaxes(cache, 1, 2)
    vmem, hbm = pl.BlockSpec(memory_space=pltpu.VMEM), pl.BlockSpec(memory_space=pltpu.HBM)
    return pl.pallas_call(
        functools.partial(attend_kernel, query_width ** (-0.5)),
        out_shape=jax.ShapeDtypeStruct((copies, BAT, (own + 1) * heads, lanes), jnp.bfloat16),
        in_specs=[vmem, vmem, vmem, hbm, hbm, hbm],
        out_specs=vmem,
        scratch_shapes=[
            pltpu.VMEM(turned.shape, turned.dtype),
            pltpu.VMEM(key.shape, key.dtype),
            pltpu.VMEM(value.shape, value.dtype),
            pltpu.VMEM((requests, heads, lanes), jnp.float32),
            pltpu.VMEM((requests, heads, latent_width), jnp.float32),
            pltpu.VMEM((requests, heads, shard_len), jnp.float32),
            pltpu.VMEM((heads, requests, latent_width), jnp.float32),
            pltpu.SemaphoreType.DMA((requests + 2,)),
        ],
        compiler_params=pltpu.CompilerParams(vmem_limit_bytes=large_grant),
        name="attend",
    )(own_heads, received, limits, turned, key, value)


def merged(tiles, stats, width):
    heads = stats.shape[1]
    maxima, totals = take_stats(stats, width)
    maxima = jnp.where(totals > 0, maxima, empty_score)
    highest = jnp.max(maxima, axis=0, keepdims=True)
    factors = jnp.exp(maxima - highest)
    total = jnp.sum(totals * factors, axis=0)
    sums = []
    for k in range(width):
        part = tiles[:, k * heads : (k + 1) * heads] * factors[:, :, k : k + 1]
        sums.append(jnp.sum(part, axis=0))
    return sums, highest[0], total


def summed(heads, pieces):
    width = pieces.shape[1] // heads - 1
    block = pieces.astype(jnp.float32)
    return merged(block[:, : width * heads], block[:, width * heads :], width)


def packed(heads, sums, highest, total):
    stats = jnp.zeros((heads, lanes), jnp.float32)
    for k in range(len(sums)):
        stats = put_stats(stats, k, len(sums), highest[:, k : k + 1], total[:, k : k + 1])
    return jnp.concatenate([*sums, stats], axis=0).astype(jnp.bfloat16)


def merge_across_kernel(heads, pieces, out):
    for b in range(BAT):
        out[b] = packed(heads, *summed(heads, pieces[:, b]))


def merge_kernel(heads, *refs):
    *parts, out = refs
    for b in range(BAT):
        out[b] = packed(heads, *summed(heads, jnp.stack([part[b] for part in parts])))


def finish_kernel(heads, *refs):
    *parts, out = refs
    here = lax.axis_index("seq_1") == root
    for b in range(BAT):
        sums, _, total = summed(heads, jnp.stack([part[b] for part in parts]))
        for k in range(len(sums)):
            result = sums[k] / total[:, k : k + 1]
            out[k, b] = jnp.where(here, result, 0.0).astype(jnp.bfloat16)


def whole(kernel, heads, shape, *operands):
    vmem = pl.BlockSpec(memory_space=pltpu.VMEM)
    return pl.pallas_call(
        functools.partial(kernel, heads),
        out_shape=jax.ShapeDtypeStruct(shape, jnp.bfloat16),
        in_specs=[vmem] * len(operands),
        out_specs=vmem,
        compiler_params=pltpu.CompilerParams(vmem_limit_bytes=small_grant),
    )(*operands)


def moved(value, pairs):
    return lax.ppermute(value, "seq_1", pairs)


def one_of(plane, planes):
    return functools.reduce(jnp.logical_or, [plane == p for p in planes])


def within(inside, step, value):
    return lax.cond(inside, step, lambda kept: kept, value)


root = 1
near_root = 2
first_sources = (3, 4, 5, 6, 7, 8)
early_sources = (near_root, 9, 10, 11)
middle_sources = (0, 12, 13)
late_sources = (14, 15)
start_order = (15, 14, 13, 12, 11, 10, 9, near_root, 0)
rounds = (
    [[(1, 3)], [(1, 2)], [(1, 0)]],
    [[(2, 5), (3, 7)], [(2, 4), (3, 6)]],
    [[(4, 9), (5, 11), (6, 13), (7, 15)], [(4, 8), (5, 10), (6, 12), (7, 14)]],
)


def takes_part(moves):
    planes = sorted({p for pairs in moves for pair in pairs for p in pair})
    return one_of(lax.axis_index("seq_1"), planes)


def gathered_at_root(in_first, partial, heads, shape):
    def merge(kept, parts):
        return whole(merge_kernel, heads, kept.shape, kept, *parts)

    partial = within(
        in_first,
        lambda kept: merge(kept, [moved(kept, [(p, near_root)]) for p in first_sources]),
        partial,
    )
    parts = {}
    for p in start_order:
        parts[p] = moved(partial, [(p, root)])
    for group in (early_sources, middle_sources):
        partial = merge(partial, [parts[p] for p in group])
    late = [parts[p] for p in late_sources]
    return whole(finish_kernel, heads, shape, partial, *late)


def handed_on(inside, result):
    def step(moves, kept):
        return functools.reduce(jnp.add, [moved(kept, pairs) for pairs in moves], kept)

    for moves, here in zip(rounds, inside):
        result = within(here, functools.partial(step, moves), result)
    return result


def per_device(queries, latent_cache, cache_lengths, key_weight, value_weight):
    heads = key_weight.shape[0]
    received = lax.ppermute(queries, "bat", [(0, 1), (1, 0)])
    in_rounds = [takes_part(moves) for moves in rounds]
    in_first = takes_part([[(p, near_root) for p in first_sources]])
    own_heads, limits = prepare(cache_lengths, queries, heads, in_first, *in_rounds)
    across = lax.axis_size("seq_0")
    partial = attend(
        own_heads, received, limits, latent_cache, key_weight, value_weight, across
    )
    shape = partial.shape
    pieces = lax.all_to_all(
        partial.reshape(across * BAT, *shape[2:]), ("seq_0", "bat"), 0, 0, tiled=True
    ).reshape(shape)
    partial = whole(merge_across_kernel, heads, shape[1:], pieces)
    own, value_width = queries.shape[0], value_weight.shape[2]
    shape = (own, BAT, heads, value_width)
    result = gathered_at_root(in_first, partial, heads, shape)
    result = handed_on(in_rounds, result)
    return result.reshape(own, BAT * heads, value_width)


def solution(mesh):
    torus = Mesh(
        mesh.devices.reshape(mesh.shape["grp"], SEQ_0, mesh.shape["seq"] // SEQ_0, mesh.shape["bat"]),
        ("grp", "seq_0", "seq_1", "bat"),
    )
    placed = (
        P(("grp", "bat"), None, None),
        P("grp", SEQ, None),
        P("grp"),
        P("bat", None, None),
        P("bat", None, None),
    )
    return jax.shard_map(
        per_device,
        mesh=torus,
        in_specs=placed,
        out_specs=P(("grp", "bat"), None, None),
        check_vma=False,
    )
```
